32 devices in a mesh: elem: 16 (over z, y, x), param: 2 (over core).
Axes of the slice: x: 2, y: 2, z: 4, core: 2. Of those that a mesh axis runs over, the one named last changes fastest.
Arguments:
- coords: bfloat16 [8, 300], P('param'), may hold values from -6 to 6
- basis_rows: bfloat16 [3, 300, 4096], P(None, None, 'elem'), may hold values from -0.375 to 0.375
- connectivity: int32 [4096, 8], P(('elem', 'param')), may hold values from 0 to 319, as said below
- modulus: float32 [4096], P(('elem', 'param')), may hold values from 0.5 to 15
- stiffness: float32 [24, 24], replicated, may hold values from -1.25 to 1.25
Outputs:
- training: bfloat16 [8, 300, 4096], P(None, None, ('elem', 'param'))
- target: float32 [8, 300], replicated
The draws below stay inside these ranges and needn't reach their ends.
Inputs may be any that keep to these rules, and one draw needn't show every extreme that they name: `connectivity`: A number c of 256 or more names node c - 256 of the next node block; the last block's next block is the first. An element's eight corner numbers lie among min(8, 64) consecutive numbers; where these lie in the block is not tied to the element's position.
All inputs are finite; a program needn't handle non-finite values.
Results may differ from the reference program's by a relative error of at most 0.0072.
Values may be sent and summed in bfloat16 or wider, within the bound.
A program may use at most 64 MiB of HBM per device.

```python
import math
import jax
import jax.numpy as jnp
from jax import lax

MODES = 300
SNAP = 8
NODE_BLK = 256
GHOST = 64
NODES = 4096
ELEMS = 4096
N_ELEM = 16


def draw_modulus(key, part):
    position = jnp.arange(ELEMS, dtype=jnp.float32)
    rising = 1.0 + 2.0 * position / max(ELEMS - 1, 1)
    factor = jnp.exp(jax.random.uniform(key, (ELEMS,), jnp.float32, math.log(0.5), math.log(5.0)))
    return (rising * factor).astype(jnp.float32)


def draw_connectivity(key, part):
    window = min(8, GHOST)
    top_base = NODE_BLK + GHOST - window
    local_pos = jnp.arange(ELEMS, dtype=jnp.int32) % NODE_BLK
    random_base = jax.random.randint(jax.random.fold_in(key, 37), (ELEMS,), 0, top_base + 1, jnp.int32)
    base_node = jnp.where(local_pos == 0, 0, jnp.where(local_pos == NODE_BLK - 1, top_base, random_base)).astype(jnp.int32)
    scores = jax.random.randint(jax.random.fold_in(key, 31), (ELEMS, 8), 0, 1 << 20, jnp.int32)
    scores = scores * 8 + jnp.arange(8, dtype=jnp.int32)[None, :]
    ordering = jnp.argsort(scores, axis=1).astype(jnp.int32)
    offsets = ordering % window
    return (base_node[:, None] + offsets).astype(jnp.int32)


def draw_basis_rows(key, part):
    spacing = 8
    cells = -(-NODES // spacing)
    coarse = jax.random.normal(jax.random.fold_in(key, 41), (3, MODES, cells + 1), jnp.float32)
    fraction = (jnp.arange(spacing, dtype=jnp.float32) + 0.5) / spacing
    spread_norm = jnp.sqrt((1.0 - fraction) ** 2 + fraction ** 2)
    smooth = (coarse[:, :, :-1, None] * (1.0 - fraction) + coarse[:, :, 1:, None] * fraction) / spread_norm
    smooth = smooth.reshape(3, MODES, cells * spacing)[:, :, :NODES]
    node_pos = (jnp.arange(NODES, dtype=jnp.int32) % NODE_BLK).astype(jnp.float32) / NODE_BLK
    node_levels = jnp.exp(jax.random.uniform(jax.random.fold_in(key, 43), (NODES,), jnp.float32, math.log(0.7), math.log(1.4)))
    rough_part = jax.random.normal(jax.random.fold_in(key, 47), (3, MODES, NODES), jnp.float32)
    amplitude = (0.7 + 0.6 * node_pos) * node_levels
    shared = 0.35 + 0.55 * node_pos
    values = amplitude * (shared * smooth + jnp.sqrt(1.0 - shared * shared) * rough_part) / math.sqrt(MODES)
    return jnp.clip(values, -0.375, 0.375).astype(jnp.bfloat16)


def level_of(rng, extent, shards, smallest, high):
    level, own = 1.0, jax.random.fold_in(rng, 6)
    for axis_at, shards_of in shards:
        steps = jnp.exp(jax.random.uniform(jax.random.fold_in(own, axis_at), (shards_of,), jnp.float32, smallest / len(shards), high / len(shards)))
        level = level * jnp.repeat(steps, extent[axis_at] // shards_of).reshape([-1 if axis == axis_at else 1 for axis in range(len(extent))])
    return level


def scatter_about(key, extent, spread, reach, shards=(), held_as=jnp.bfloat16):
    loudness = level_of(key, extent, shards, -0.22, 0.18) if shards else 1.0
    values = jax.random.normal(key, extent, jnp.float32) * spread * loudness
    return jnp.minimum(jnp.maximum(values, -reach), reach).astype(held_as)


def setup_inputs(seed: int = 0) -> dict:
    key_of = jax.random.split(jax.random.key(seed), 6)
    coords = scatter_about(key_of[0], (SNAP, MODES), 1.0, 6.0, ((0, 2),))
    basis_rows = draw_basis_rows(jax.random.fold_in(key_of[5], 71), 0)
    connectivity = draw_connectivity(jax.random.fold_in(key_of[5], 71), 0)
    modulus = draw_modulus(jax.random.fold_in(key_of[5], 71), 0)
    stiffness = scatter_about(key_of[4], (24, 24), 24 ** -0.5, 1.25, (), jnp.float32)
    return {"coords": coords, "basis_rows": basis_rows, "connectivity": connectivity, "modulus": modulus, "stiffness": stiffness}


def block_columns(displaced, basis_rows, stiffness, corner_ids, mod_block):
    index_table = corner_ids.T
    count = index_table.shape[1]
    snaps = displaced.shape[0]
    corner_disp = displaced[:, :, index_table].reshape(snaps, 24, count).astype(jnp.float32)
    linear = jnp.einsum('kj,sje->ske', stiffness, corner_disp, precision=lax.Precision.HIGHEST)
    forces = (mod_block * (linear + 0.25 * corner_disp * corner_disp * corner_disp)).astype(jnp.bfloat16)
    forces = forces.reshape(snaps, 3, 8, count)
    element_basis = basis_rows[:, :, index_table]
    return jnp.einsum('cmae,scae->sme', element_basis.astype(jnp.float32), forces.astype(jnp.float32), precision=lax.Precision.HIGHEST)

def global_ids(block_id, conn_block):
    following = (block_id + 1) % N_ELEM
    return jnp.where(conn_block < NODE_BLK, block_id * NODE_BLK + conn_block, following * NODE_BLK + conn_block - NODE_BLK).astype(jnp.int32)

def reference(coords, basis_rows, connectivity, modulus, stiffness):
    displaced = jnp.stack([jnp.dot(coords, basis_rows[component], preferred_element_type=jnp.float32) for component in range(3)], axis=1).astype(jnp.bfloat16)
    conn_blocks = connectivity.reshape(N_ELEM, NODE_BLK, 8)
    mod_blocks = modulus.reshape(N_ELEM, NODE_BLK)
    block_ids = jnp.arange(N_ELEM, dtype=jnp.int32)

    def block_stats(inputs):
        block_id, conn_block, mod_block = inputs
        columns = block_columns(displaced, basis_rows, stiffness, global_ids(block_id, conn_block), mod_block)
        return (lax.optimization_barrier(jnp.sum(jnp.sqrt(lax.optimization_barrier(jnp.sum(columns * columns, axis=1))), axis=1)), lax.optimization_barrier(jnp.sum(columns, axis=2)))
    norm_parts, force_parts = lax.map(block_stats, (block_ids, conn_blocks, mod_blocks))
    row_scale = lax.optimization_barrier(jnp.sum(norm_parts, axis=0)) / ELEMS
    target = lax.optimization_barrier(jnp.sum(force_parts, axis=0)) / (row_scale[:, None] * math.sqrt(ELEMS))

    def block_output(inputs):
        block_id, conn_block, mod_block = inputs
        columns = block_columns(displaced, basis_rows, stiffness, global_ids(block_id, conn_block), mod_block)
        return (columns / row_scale[:, None, None]).astype(jnp.bfloat16)
    pieces = lax.map(block_output, (block_ids, conn_blocks, mod_blocks))
    training = jnp.transpose(pieces, (1, 2, 0, 3)).reshape(SNAP, MODES, ELEMS)
    return (training, target)
```

```python
import functools
import math

import jax
import jax.numpy as jnp
from jax import lax
from jax.experimental import pallas as pl
from jax.experimental.pallas import tpu as pltpu
from jax.sharding import PartitionSpec as P

MESH = pl.DeviceIdType.MESH
F32 = jnp.float32
BF16 = jnp.bfloat16


def round_up(value, to):
    return -(-value // to) * to


def kernel(
    elems, params, inner,
    coords_ref, basis_ref, conn_ref, mod_ref, stiff_ref,
    cols_ref, target_ref, scale_ref,
    packed, ghost_in, ghost, all_coords, disp, mask, weights, part, part_p, part_i, part_o,
    send_g, recv_g, send_c, recv_c, send_p, recv_p, send_i, recv_i, send_o, recv_o,
):
    outer = elems // inner
    own_snaps, modes = coords_ref.shape
    snaps = own_snaps * params
    nodes = basis_ref.shape[2]
    ghosts = nodes // 4
    total_nodes = nodes + ghosts
    count = conn_ref.shape[0]
    me_e, me_p = lax.axis_index("elem"), lax.axis_index("param")
    me_i, me_o = me_e % inner, me_e // inner
    before, after = (me_e + elems - 1) % elems, (me_e + 1) % elems

    def peers(me, size):
        return [((me + j) % size, (me + size - j) % size) for j in range(1, size)]

    def inner_id(i):
        return (me_o * inner + i, me_p)

    def outer_id(o):
        return (o * inner + me_i, me_p)

    barrier = pltpu.get_barrier_semaphore()
    near = [(before, me_p), (after, me_p)]
    near += [(me_e, to) for to, _ in peers(me_p, params)]
    near += [inner_id(to) for to, _ in peers(me_i, inner)]
    near += [outer_id(to) for to, _ in peers(me_o, outer)]
    for device in near:
        pl.semaphore_signal(barrier, inc=1, device_id=device, device_id_type=MESH)

    half = packed.shape[1]
    split = half < modes
    if split:
        for k in range(3):
            packed[k, :, :ghosts] = basis_ref[k, :half, :ghosts]
            packed[k, : modes - half, ghosts:] = basis_ref[k, half:, :ghosts]
    else:
        for k in range(3):
            packed[k, :modes] = basis_ref[k, :, :ghosts]
    padded = all_coords.shape[2]
    all_coords[me_p, :own_snaps, :modes] = coords_ref[...].astype(F32)

    pl.semaphore_wait(barrier, len(near))
    ghost_copy = pltpu.make_async_remote_copy(
        src_ref=packed, dst_ref=ghost_in, send_sem=send_g, recv_sem=recv_g,
        device_id=(before, me_p), device_id_type=MESH,
    )
    ghost_copy.start()

    def exchange(ref, me, size, device_of, send, recv):
        copies = []
        for j, (to, source) in enumerate(peers(me, size)):
            out = pltpu.make_async_remote_copy(
                src_ref=ref.at[me], dst_ref=ref.at[me], send_sem=send.at[j], recv_sem=recv.at[me],
                device_id=device_of(to), device_id_type=MESH,
            )
            out.start()
            came = pltpu.make_async_remote_copy(
                src_ref=ref.at[source], dst_ref=ref.at[source], send_sem=send.at[j],
                recv_sem=recv.at[source], device_id=device_of(to), device_id_type=MESH,
            )
            copies.append((out, came))
        return copies

    def finish(copies):
        for out, came in copies:
            came.wait_recv()
        for out, came in copies:
            out.wait_send()

    coord_copies = exchange(all_coords, me_p, params, lambda p: (me_e, p), send_c, recv_c)

    corners = jnp.transpose(conn_ref[...])
    base = jnp.min(corners, axis=0, keepdims=True)
    residue = corners % 8
    lane_at = corners % 128
    tile_at = corners // 128
    node = lax.broadcasted_iota(jnp.int32, (total_nodes, count), 0)
    inside = (node >= base) & (node < base + 8)
    mask[...] = jnp.where(inside, 1.0, 0.0).astype(BF16)
    stiff = stiff_ref[...]
    high = stiff.astype(BF16)
    rest = stiff - high.astype(F32)
    mid = rest.astype(BF16)
    low = (rest - mid.astype(F32)).astype(BF16)
    modulus = mod_ref[...]
    modulus2 = jnp.concatenate([modulus, modulus], axis=1)

    finish(coord_copies)
    full_coords = jnp.concatenate(
        [all_coords[p, :own_snaps, :modes] for p in range(params)], axis=0
    ).astype(BF16)
    own_tiles = nodes // 128
    for k in range(3):
        moved = jnp.dot(full_coords, basis_ref[k], preferred_element_type=F32)
        moved = moved.astype(BF16).astype(F32)
        for t in range(own_tiles):
            disp[t, k] = moved[:, t * 128 : (t + 1) * 128]

    ghost_copy.wait_recv()
    for k in range(3):
        if split:
            ghost[:half, k * ghosts : (k + 1) * ghosts] = ghost_in[k, :, :ghosts]
            ghost[half:, k * ghosts : (k + 1) * ghosts] = ghost_in[k, : modes - half, ghosts:]
        else:
            ghost[:, k * ghosts : (k + 1) * ghosts] = ghost_in[k, :modes]
    moved = jnp.dot(full_coords, ghost[...], preferred_element_type=F32).astype(BF16).astype(F32)
    ghost_tiles = disp.shape[0] - own_tiles
    for k in range(3):
        for t in range(ghost_tiles):
            width = min(128, ghosts)
            disp[own_tiles + t, k, :, :width] = moved[:, k * ghosts + t * 128 :][:, :width]

    lane = lax.broadcasted_iota(jnp.int32, (1, 128), 1)
    row8 = lax.broadcasted_iota(jnp.int32, (8, count), 0)

    def one_pair(p, sums):
        pieces = []
        for at in range(2):
            rows = []
            for k in range(3):
                found = jnp.zeros((8, count), F32)
                for t in range(disp.shape[0]):
                    line = jnp.broadcast_to(disp[t, k, pl.ds(2 * p + at, 1), :], (8, 128))
                    got = jnp.take_along_axis(line, lane_at, axis=1)
                    found = jnp.where(tile_at == t, got, found)
                rows.append(found)
            pieces.append(jnp.concatenate(rows, axis=0))
        moved = jnp.concatenate(pieces, axis=1)
        moved16 = moved.astype(BF16)
        linear = jnp.dot(low, moved16, preferred_element_type=F32)
        linear = linear + jnp.dot(mid, moved16, preferred_element_type=F32)
        linear = linear + jnp.dot(high, moved16, preferred_element_type=F32)
        forces = (modulus2 * (linear + 0.25 * moved * moved * moved)).astype(BF16).astype(F32)
        for at in range(2):
            for k in range(3):
                spread = jnp.zeros((8, count), F32)
                for a in range(8):
                    force = forces[k * 8 + a : k * 8 + a + 1, at * count : (at + 1) * count]
                    spread = spread + jnp.where(residue[a : a + 1] == row8, force, 0.0)
                twice = jnp.concatenate([spread, spread], axis=0).astype(BF16)
                tall = jnp.concatenate([twice] * (total_nodes // 16), axis=0) * mask[...]
                columns = slice(at * count, (at + 1) * count)
                weights[k * nodes : (k + 1) * nodes, columns] = tall[:nodes]
                start = 3 * nodes + k * ghosts
                weights[start : start + ghosts, columns] = tall[nodes:]
        result = jnp.dot(ghost[...], weights[3 * nodes :], preferred_element_type=F32)
        for k in range(3):
            result = result + jnp.dot(
                basis_ref[k], weights[k * nodes : (k + 1) * nodes], preferred_element_type=F32
            )
        for at in range(2):
            s = 2 * p + at
            mine = result[:, at * count : (at + 1) * count]
            cols_ref[s] = mine
            norm = jnp.sqrt(jnp.sum(mine * mine, axis=0, keepdims=True))
            norm = jnp.sum(norm, axis=1, keepdims=True)
            line = jnp.concatenate([jnp.sum(mine, axis=1, keepdims=True), norm], axis=0)
            sums = jnp.where(lane == s, line, sums)
        return sums

    sums = jnp.zeros((modes + 1, 128), F32)
    if snaps <= 8:
        for p in range(snaps // 2):
            sums = one_pair(p, sums)
    else:
        sums = lax.fori_loop(0, snaps // 2, one_pair, sums)
    wide = part_p.shape[2]
    part[...] = jnp.zeros_like(part)
    part[: modes + 1] = sums
    flat = jnp.concatenate(
        [jnp.transpose(part[t * 128 : (t + 1) * 128])[:snaps] for t in range(wide // 128)], axis=1
    )
    ghost_copy.wait_send()

    def reduced(value, ref, me, size, device_of, send, recv):
        ref[me] = value
        finish(exchange(ref, me, size, device_of, send, recv))
        total = ref[0]
        for j in range(1, size):
            total = total + ref[j]
        return total

    flat = reduced(flat, part_p, me_p, params, lambda p: (me_e, p), send_p, recv_p)
    flat = reduced(flat, part_i, me_i, inner, inner_id, send_i, recv_i)
    flat = reduced(flat, part_o, me_o, outer, outer_id, send_o, recv_o)
    elem_total = count * elems * params
    row_scale = flat[:, modes : modes + 1] / elem_total
    target_ref[...] = flat[:, :modes] / (row_scale * math.sqrt(elem_total))
    scale_ref[...] = jnp.broadcast_to(1.0 / row_scale, scale_ref.shape)


def local(elems, params, coords, basis_rows, connectivity, modulus, stiffness):
    own_snaps, modes = coords.shape
    nodes = basis_rows.shape[2]
    count = connectivity.shape[0]
    snaps = own_snaps * params
    ghosts = nodes // 4
    inner = 4 if elems % 4 == 0 else elems
    outer = elems // inner
    half, across = (modes, ghosts) if ghosts % 128 == 0 else (round_up(-(-modes // 2), 32), 2 * ghosts)
    tall = round_up(half, 16)
    tiles = nodes // 128 + -(-ghosts // 128)
    wide = round_up(modes + 1, 128)
    dma = pltpu.SemaphoreType.DMA
    vmem = pl.BlockSpec(memory_space=pltpu.VMEM)
    cols, target, scale = pl.pallas_call(
        functools.partial(kernel, elems, params, inner),
        out_shape=(
            jax.ShapeDtypeStruct((snaps, modes, count), F32),
            jax.ShapeDtypeStruct((snaps, modes), F32),
            jax.ShapeDtypeStruct((snaps, 128), F32),
        ),
        in_specs=[vmem] * 5,
        out_specs=(vmem, vmem, vmem),
        scratch_shapes=[
            pltpu.VMEM((3, tall, across), BF16),
            pltpu.VMEM((3, tall, across), BF16),
            pltpu.VMEM((modes, 3 * ghosts), BF16),
            pltpu.VMEM((params, round_up(own_snaps, 8), round_up(modes, 128)), F32),
            pltpu.VMEM((tiles, 3, snaps, 128), F32),
            pltpu.VMEM((nodes + ghosts, count), BF16),
            pltpu.VMEM((3 * (nodes + ghosts), 2 * count), BF16),
            pltpu.VMEM((wide, 128), F32),
            pltpu.VMEM((params, snaps, wide), F32),
            pltpu.VMEM((inner, snaps, wide), F32),
            pltpu.VMEM((outer, snaps, wide), F32),
            dma, dma,
            dma((params,)), dma((params,)),
            dma((params,)), dma((params,)),
            dma((inner,)), dma((inner,)),
            dma((outer,)), dma((outer,)),
        ],
        compiler_params=pltpu.CompilerParams(
            collective_id=0, has_side_effects=True, vmem_limit_bytes=48 * 1024 * 1024
        ),
    )(coords, basis_rows, connectivity, modulus.reshape(1, count), stiffness)
    training = (cols * scale[:, :1, None]).astype(BF16)
    return (training, target)


def solution(mesh):
    in_specs = (
        P("param", None),
        P(None, None, "elem"),
        P(("elem", "param"), None),
        P(("elem", "param")),
        P(),
    )
    out_specs = (P(None, None, ("elem", "param")), P())
    run = functools.partial(local, mesh.shape["elem"], mesh.shape["param"])
    return jax.shard_map(run, mesh=mesh, in_specs=in_specs, out_specs=out_specs, check_vma=False)
```

```python
import functools
import math

import jax
import jax.numpy as jnp
from jax import lax
from jax.experimental import pallas as pl
from jax.experimental.pallas import tpu as pltpu
from jax.sharding import PartitionSpec as P

MESH = pl.DeviceIdType.MESH
F32 = jnp.float32
BF16 = jnp.bfloat16


def round_up(value, to):
    return -(-value // to) * to


def kernel(
    elems, params, inner,
    coords_hbm, basis_hbm, conn_hbm, mod_hbm, stiff_hbm,
    cols_ref, flat_ref,
    coords_ref, basis_ref, conn_ref, mod_ref, stiff_ref,
    packed, ghost_in, ghost, disp, mask, weights, ghost_weights, acc, part, part_p, part_i, part_o,
    load, send_g, recv_g, send_d, recv_d, send_n, recv_n, send_p, recv_p, send_i, recv_i, send_o, recv_o,
):
    outer = elems // inner
    own_snaps, modes = coords_ref.shape
    snaps = own_snaps * params
    nodes = basis_hbm.shape[2]
    ghosts = nodes // 4
    total_nodes = nodes + ghosts
    count = conn_ref.shape[1]
    me_e, me_p = lax.axis_index("elem"), lax.axis_index("param")
    me_i, me_o = me_e % inner, me_e // inner
    before, after = (me_e + elems - 1) % elems, (me_e + 1) % elems

    def peers(me, size):
        return [((me + j) % size, (me + size - j) % size) for j in range(1, size)]

    def inner_id(i):
        return (me_o * inner + i, me_p)

    def outer_id(o):
        return (o * inner + me_i, me_p)

    barrier = pltpu.get_barrier_semaphore()
    near = [(before, p) for p in range(params)] + [(after, p) for p in range(params)]
    near += [(me_e, to) for to, _ in peers(me_p, params)]
    near += [inner_id(to) for to, _ in peers(me_i, inner)]
    near += [outer_id(to) for to, _ in peers(me_o, outer)]
    for device in near:
        pl.semaphore_signal(barrier, inc=1, device_id=device, device_id_type=MESH)

    loads = [(coords_hbm, coords_ref)]
    loads += [(basis_hbm.at[k], basis_ref.at[:, pl.ds(k * nodes, nodes)]) for k in range(3)]
    loads += [(conn_hbm, conn_ref), (mod_hbm, mod_ref), (stiff_hbm, stiff_ref)]
    loads = [pltpu.make_async_copy(src, dst, load.at[i]) for i, (src, dst) in enumerate(loads)]
    for copy in loads:
        copy.start()

    def remote(src, dst, send, recv, device):
        return pltpu.make_async_remote_copy(
            src_ref=src, dst_ref=dst, send_sem=send, recv_sem=recv,
            device_id=device, device_id_type=MESH,
        )

    own_tiles = nodes // 128
    ghost_tiles = disp.shape[1] - own_tiles
    half = packed.shape[1]
    split = half < modes
    loads[0].wait()
    for k in range(3):
        loads[1 + k].wait()
        moved = jnp.dot(
            coords_ref[...], basis_ref[:, k * nodes : (k + 1) * nodes], preferred_element_type=F32
        )
        moved = moved.astype(BF16).astype(F32)
        for t in range(own_tiles):
            disp[me_p, t, k] = moved[:, t * 128 : (t + 1) * 128]
    for k in range(3):
        at = k * nodes
        if split:
            packed[k, :, :ghosts] = basis_ref[:half, at : at + ghosts]
            packed[k, : modes - half, ghosts:] = basis_ref[half:, at : at + ghosts]
        else:
            packed[k, :modes] = basis_ref[:, at : at + ghosts]

    pl.semaphore_wait(barrier, len(near))
    own_part, ghost_part = pl.ds(0, own_tiles), pl.ds(own_tiles, ghost_tiles)
    sends, arrivals = [], []
    for p in range(params):
        turn = (me_p + p) % params
        source = (me_p + params - p) % params
        sends.append(remote(
            disp.at[me_p, pl.ds(0, ghost_tiles)], disp.at[me_p, ghost_part],
            send_d.at[p], recv_d.at[me_p], (before, turn),
        ))
        arrivals.append(remote(
            disp.at[source, pl.ds(0, ghost_tiles)], disp.at[source, ghost_part],
            send_d.at[p], recv_d.at[source], (before, turn),
        ))
        if p:
            sends.append(remote(
                disp.at[me_p, own_part], disp.at[me_p, own_part],
                send_n.at[p], recv_n.at[me_p], (me_e, turn),
            ))
            arrivals.append(remote(
                disp.at[source, own_part], disp.at[source, own_part],
                send_n.at[p], recv_n.at[source], (me_e, turn),
            ))
    ghost_copy = remote(packed, ghost_in, send_g, recv_g, (before, me_p))
    for copy in sends + [ghost_copy]:
        copy.start()

    for copy in loads[4:]:
        copy.wait()
    corners = conn_ref[...]
    base = jnp.min(corners, axis=0, keepdims=True)
    residue = corners % 8
    lane_at = corners % 128
    tile_at = corners // 128
    node = lax.broadcasted_iota(jnp.int32, (total_nodes, count), 0)
    inside = (node >= base) & (node < base + 8)
    mask[...] = jnp.where(inside, 1.0, 0.0).astype(BF16)
    stiff = stiff_ref[...]
    high = stiff.astype(BF16)
    rest = stiff - high.astype(F32)
    mid = rest.astype(BF16)
    low = (rest - mid.astype(F32)).astype(BF16)
    modulus = mod_ref[...]
    modulus2 = jnp.concatenate([modulus, modulus], axis=1)
    part[...] = jnp.zeros_like(part)
    lane = lax.broadcasted_iota(jnp.int32, (1, 128), 1)
    row8 = lax.broadcasted_iota(jnp.int32, (8, count), 0)

    for copy in arrivals:
        copy.wait_recv()

    def own_product(p):
        pieces = []
        for at in range(2):
            s = 2 * p + at
            rows = []
            for k in range(3):
                found = jnp.zeros((8, count), F32)
                for t in range(disp.shape[1]):
                    line = disp[s // own_snaps, t, k, pl.ds(s % own_snaps, 1), :]
                    got = jnp.take_along_axis(jnp.broadcast_to(line, (8, 128)), lane_at, axis=1)
                    found = jnp.where(tile_at == t, got, found)
                rows.append(found)
            pieces.append(jnp.concatenate(rows, axis=0))
        moved = jnp.concatenate(pieces, axis=1)
        moved16 = moved.astype(BF16)
        linear = jnp.dot(low, moved16, preferred_element_type=F32)
        linear = linear + jnp.dot(mid, moved16, preferred_element_type=F32)
        linear = linear + jnp.dot(high, moved16, preferred_element_type=F32)
        forces = (modulus2 * (linear + 0.25 * moved * moved * moved)).astype(BF16).astype(F32)
        for at in range(2):
            for k in range(3):
                spread = jnp.zeros((8, count), F32)
                for a in range(8):
                    force = forces[k * 8 + a : k * 8 + a + 1, at * count : (at + 1) * count]
                    spread = spread + jnp.where(residue[a : a + 1] == row8, force, 0.0)
                twice = jnp.concatenate([spread, spread], axis=0).astype(BF16)
                tall = jnp.concatenate([twice] * (total_nodes // 16), axis=0) * mask[...]
                columns = slice(at * count, (at + 1) * count)
                weights[k * nodes : (k + 1) * nodes, columns] = tall[:nodes]
                ghost_weights[p, k * ghosts : (k + 1) * ghosts, columns] = tall[nodes:]
        acc[p] = jnp.dot(basis_ref[...], weights[...], preferred_element_type=F32)

    def whole_product(p, sums):
        result = acc[p] + jnp.dot(ghost[...], ghost_weights[p], preferred_element_type=F32)
        for at in range(2):
            s = 2 * p + at
            mine = result[:, at * count : (at + 1) * count]
            cols_ref[pl.ds(s, modes, stride=snaps), :] = mine
            norm = jnp.sqrt(jnp.sum(mine * mine, axis=0, keepdims=True))
            norm = jnp.sum(norm, axis=1, keepdims=True)
            line = jnp.concatenate([jnp.sum(mine, axis=1, keepdims=True), norm], axis=0)
            sums = jnp.where(lane == s, line, sums)
        return sums

    pairs = snaps // 2
    if pairs <= 4:
        for p in range(pairs):
            own_product(p)
    else:
        lax.fori_loop(0, pairs, lambda p, c: (own_product(p), c)[1], 0)

    ghost_copy.wait_recv()
    for k in range(3):
        if split:
            ghost[:half, k * ghosts : (k + 1) * ghosts] = ghost_in[k, :, :ghosts]
            ghost[half:, k * ghosts : (k + 1) * ghosts] = ghost_in[k, : modes - half, ghosts:]
        else:
            ghost[:, k * ghosts : (k + 1) * ghosts] = ghost_in[k, :modes]
    sums = jnp.zeros((modes + 1, 128), F32)
    if pairs <= 4:
        for p in range(pairs):
            sums = whole_product(p, sums)
    else:
        sums = lax.fori_loop(0, pairs, whole_product, sums)

    wide = part_p.shape[2]
    part[: modes + 1] = sums
    flat = jnp.concatenate(
        [jnp.transpose(part[t * 128 : (t + 1) * 128])[:snaps] for t in range(wide // 128)], axis=1
    )
    waits = sends + [ghost_copy]

    def reduced(value, ref, me, size, device_of, send, recv):
        ref[me] = value
        arriving = []
        for j, (to, source) in enumerate(peers(me, size)):
            out = remote(ref.at[me], ref.at[me], send.at[j], recv.at[me], device_of(to))
            out.start()
            waits.append(out)
            arriving.append(remote(
                ref.at[source], ref.at[source], send.at[j], recv.at[source], device_of(to)
            ))
        for copy in arriving:
            copy.wait_recv()
        total = ref[0]
        for j in range(1, size):
            total = total + ref[j]
        return total

    flat = reduced(flat, part_p, me_p, params, lambda p: (me_e, p), send_p, recv_p)
    flat = reduced(flat, part_i, me_i, inner, inner_id, send_i, recv_i)
    flat = reduced(flat, part_o, me_o, outer, outer_id, send_o, recv_o)
    flat_ref[...] = flat
    for copy in waits:
        copy.wait_send()


def finish_kernel(elem_total, cols_ref, flat_ref, training_hbm, target_hbm, training, target, sem):
    snaps, modes = target.shape
    row_scale = flat_ref[:, modes : modes + 1] / elem_total
    target[...] = flat_ref[:, :modes] / (row_scale * math.sqrt(elem_total))
    copies = [pltpu.make_async_copy(target, target_hbm, sem.at[0])]
    copies[0].start()
    inverse = jnp.broadcast_to(1.0 / row_scale, (snaps, training.shape[2]))
    chunks = sem.shape[0] - 1
    size = modes // chunks
    for c in range(chunks):
        piece = cols_ref[c * size * snaps : (c + 1) * size * snaps]
        piece = piece.reshape(size, snaps, training.shape[2]) * inverse[None]
        training[c * size : (c + 1) * size] = piece.astype(BF16)
        rows = pl.ds(c * size, size)
        copies.append(pltpu.make_async_copy(training.at[rows], training_hbm.at[rows], sem.at[c + 1]))
        copies[-1].start()
    for copy in copies:
        copy.wait()


def local(elems, params, coords, basis_rows, connectivity, modulus, stiffness):
    own_snaps, modes = coords.shape
    nodes = basis_rows.shape[2]
    count = connectivity.shape[0]
    snaps = own_snaps * params
    ghosts = nodes // 4
    inner = 4 if elems % 4 == 0 else elems
    outer = elems // inner
    half, across = (modes, ghosts) if ghosts % 128 == 0 else (round_up(-(-modes // 2), 32), 2 * ghosts)
    tiles = nodes // 128 + -(-ghosts // 128)
    wide = round_up(modes + 1, 128)
    dma = pltpu.SemaphoreType.DMA
    vmem = pl.BlockSpec(memory_space=pltpu.VMEM)
    hbm = pl.BlockSpec(memory_space=pltpu.HBM)
    cols, flat = pl.pallas_call(
        functools.partial(kernel, elems, params, inner),
        out_shape=(
            jax.ShapeDtypeStruct((modes * snaps, count), F32),
            jax.ShapeDtypeStruct((snaps, wide), F32),
        ),
        in_specs=[hbm] * 5,
        out_specs=(vmem, vmem),
        scratch_shapes=[
            pltpu.VMEM((own_snaps, modes), BF16),
            pltpu.VMEM((modes, 3 * nodes), BF16),
            pltpu.VMEM((8, count), jnp.int32),
            pltpu.VMEM((1, count), F32),
            pltpu.VMEM(stiffness.shape, F32),
            pltpu.VMEM((3, round_up(half, 16), across), BF16),
            pltpu.VMEM((3, round_up(half, 16), across), BF16),
            pltpu.VMEM((modes, 3 * ghosts), BF16),
            pltpu.VMEM((params, tiles, 3, own_snaps, 128), F32),
            pltpu.VMEM((nodes + ghosts, count), BF16),
            pltpu.VMEM((3 * nodes, 2 * count), BF16),
            pltpu.VMEM((snaps // 2, 3 * ghosts, 2 * count), BF16),
            pltpu.VMEM((snaps // 2, modes, 2 * count), F32),
            pltpu.VMEM((wide, 128), F32),
            pltpu.VMEM((params, snaps, wide), F32),
            pltpu.VMEM((inner, snaps, wide), F32),
            pltpu.VMEM((outer, snaps, wide), F32),
            dma((7,)), dma, dma,
            dma((params,)), dma((params,)),
            dma((params,)), dma((params,)),
            dma((params,)), dma((params,)),
            dma((inner,)), dma((inner,)),
            dma((outer,)), dma((outer,)),
        ],
        compiler_params=pltpu.CompilerParams(
            collective_id=0, has_side_effects=True, vmem_limit_bytes=44 * 1024 * 1024
        ),
    )(coords, basis_rows, connectivity.T, modulus.reshape(1, count), stiffness)
    chunks = next(c for c in (4, 3, 2, 1) if modes % c == 0)
    training, target = pl.pallas_call(
        functools.partial(finish_kernel, count * elems * params),
        out_shape=(
            jax.ShapeDtypeStruct((modes, snaps, count), BF16),
            jax.ShapeDtypeStruct((snaps, modes), F32),
        ),
        in_specs=[vmem, vmem],
        out_specs=(hbm, hbm),
        scratch_shapes=[
            pltpu.VMEM((modes, snaps, count), BF16),
            pltpu.VMEM((snaps, modes), F32),
            dma((chunks + 1,)),
        ],
        compiler_params=pltpu.CompilerParams(vmem_limit_bytes=20 * 1024 * 1024),
    )(cols, flat)
    return (jnp.transpose(training, (1, 0, 2)), target)


def solution(mesh):
    in_specs = (
        P("param", None),
        P(None, None, "elem"),
        P(("elem", "param"), None),
        P(("elem", "param")),
        P(),
    )
    out_specs = (P(None, None, ("elem", "param")), P())
    run = functools.partial(local, mesh.shape["elem"], mesh.shape["param"])
    return jax.shard_map(run, mesh=mesh, in_specs=in_specs, out_specs=out_specs, check_vma=False)
```

```python
import functools
import math

import jax
import jax.numpy as jnp
from jax import lax
from jax.experimental import pallas as pl
from jax.experimental.pallas import tpu as pltpu
from jax.sharding import PartitionSpec as P

MESH = pl.DeviceIdType.MESH
F32 = jnp.float32
BF16 = jnp.bfloat16


def round_up(value, to):
    return -(-value // to) * to


def kernel(
    elems, params, inner,
    own_snaps, modes, dofs,
    small_ref, basis_hbm,
    cols_ref, flat_ref,
    basis_ref,
    packed, ghost_in, ghost, disp, mask, weights, ghost_weights, acc, part, part_p, part_i, part_o,
    load, send_g, recv_g, send_d, recv_d, send_n, recv_n, send_p, recv_p, send_i, recv_i, send_o, recv_o,
):
    outer = elems // inner
    snaps = own_snaps * params
    nodes = basis_hbm.shape[2]
    ghosts = nodes // 4
    total_nodes = nodes + ghosts
    count = cols_ref.shape[1]
    me_e, me_p = lax.axis_index("elem"), lax.axis_index("param")
    me_i, me_o = me_e % inner, me_e // inner
    before, after = (me_e + elems - 1) % elems, (me_e + 1) % elems

    def peers(me, size):
        return [((me + j) % size, (me + size - j) % size) for j in range(1, size)]

    def inner_id(i):
        return (me_o * inner + i, me_p)

    def outer_id(o):
        return (o * inner + me_i, me_p)

    barrier = pltpu.get_barrier_semaphore()
    near = [(before, p) for p in range(params)] + [(after, p) for p in range(params)]
    near += [(me_e, to) for to, _ in peers(me_p, params)]
    near += [inner_id(to) for to, _ in peers(me_i, inner)]
    near += [outer_id(to) for to, _ in peers(me_o, outer)]
    for device in near:
        pl.semaphore_signal(barrier, inc=1, device_id=device, device_id_type=MESH)

    loads = [
        pltpu.make_async_copy(
            basis_hbm.at[k], basis_ref.at[:, pl.ds(k * nodes, nodes)], load.at[k]
        )
        for k in range(3)
    ]
    for copy in loads:
        copy.start()

    def remote(src, dst, send, recv, device):
        return pltpu.make_async_remote_copy(
            src_ref=src, dst_ref=dst, send_sem=send, recv_sem=recv,
            device_id=device, device_id_type=MESH,
        )

    own_tiles = nodes // 128
    ghost_tiles = disp.shape[1] - own_tiles
    half = packed.shape[1]
    split = half < modes
    conn_at, mod_at, coords_at = dofs, dofs + 8, dofs + 16
    coords = small_ref[coords_at : coords_at + own_snaps, :modes].astype(BF16)
    for k in range(3):
        loads[k].wait()
        moved = jnp.dot(
            coords, basis_ref[:, k * nodes : (k + 1) * nodes], preferred_element_type=F32
        )
        moved = moved.astype(BF16).astype(F32)
        for t in range(own_tiles):
            disp[me_p, t, k] = moved[:, t * 128 : (t + 1) * 128]
    for k in range(3):
        at = k * nodes
        if split:
            packed[k, :, :ghosts] = basis_ref[:half, at : at + ghosts]
            packed[k, : modes - half, ghosts:] = basis_ref[half:, at : at + ghosts]
        else:
            packed[k, :modes] = basis_ref[:, at : at + ghosts]

    pl.semaphore_wait(barrier, len(near))
    own_part, ghost_part = pl.ds(0, own_tiles), pl.ds(own_tiles, ghost_tiles)
    sends, arrivals = [], []
    for p in range(params):
        turn = (me_p + p) % params
        source = (me_p + params - p) % params
        sends.append(remote(
            disp.at[me_p, pl.ds(0, ghost_tiles)], disp.at[me_p, ghost_part],
            send_d.at[p], recv_d.at[me_p], (before, turn),
        ))
        arrivals.append(remote(
            disp.at[source, pl.ds(0, ghost_tiles)], disp.at[source, ghost_part],
            send_d.at[p], recv_d.at[source], (before, turn),
        ))
        if p:
            sends.append(remote(
                disp.at[me_p, own_part], disp.at[me_p, own_part],
                send_n.at[p], recv_n.at[me_p], (me_e, turn),
            ))
            arrivals.append(remote(
                disp.at[source, own_part], disp.at[source, own_part],
                send_n.at[p], recv_n.at[source], (me_e, turn),
            ))
    ghost_copy = remote(packed, ghost_in, send_g, recv_g, (before, me_p))
    for copy in sends + [ghost_copy]:
        copy.start()

    corners = small_ref[conn_at : conn_at + 8, :count].astype(jnp.int32)
    base = jnp.min(corners, axis=0, keepdims=True)
    residue = corners % 8
    lane_at = corners % 128
    tile_at = corners // 128
    node = lax.broadcasted_iota(jnp.int32, (total_nodes, count), 0)
    inside = (node >= base) & (node < base + 8)
    mask[...] = jnp.where(inside, 1.0, 0.0).astype(BF16)
    stiff = small_ref[:dofs, :dofs]
    high = stiff.astype(BF16)
    rest = stiff - high.astype(F32)
    mid = rest.astype(BF16)
    low = (rest - mid.astype(F32)).astype(BF16)
    modulus = small_ref[mod_at : mod_at + 1, :count]
    modulus2 = jnp.concatenate([modulus, modulus], axis=1)
    part[...] = jnp.zeros_like(part)
    lane = lax.broadcasted_iota(jnp.int32, (1, 128), 1)
    row8 = lax.broadcasted_iota(jnp.int32, (8, count), 0)

    for copy in arrivals:
        copy.wait_recv()

    def own_product(p):
        pieces = []
        for at in range(2):
            s = 2 * p + at
            rows = []
            for k in range(3):
                found = jnp.zeros((8, count), F32)
                for t in range(disp.shape[1]):
                    line = disp[s // own_snaps, t, k, pl.ds(s % own_snaps, 1), :]
                    got = jnp.take_along_axis(jnp.broadcast_to(line, (8, 128)), lane_at, axis=1)
                    found = jnp.where(tile_at == t, got, found)
                rows.append(found)
            pieces.append(jnp.concatenate(rows, axis=0))
        moved = jnp.concatenate(pieces, axis=1)
        moved16 = moved.astype(BF16)
        linear = jnp.dot(low, moved16, preferred_element_type=F32)
        linear = linear + jnp.dot(mid, moved16, preferred_element_type=F32)
        linear = linear + jnp.dot(high, moved16, preferred_element_type=F32)
        forces = (modulus2 * (linear + 0.25 * moved * moved * moved)).astype(BF16).astype(F32)
        for at in range(2):
            for k in range(3):
                spread = jnp.zeros((8, count), F32)
                for a in range(8):
                    force = forces[k * 8 + a : k * 8 + a + 1, at * count : (at + 1) * count]
                    spread = spread + jnp.where(residue[a : a + 1] == row8, force, 0.0)
                twice = jnp.concatenate([spread, spread], axis=0).astype(BF16)
                tall = jnp.concatenate([twice] * (total_nodes // 16), axis=0) * mask[...]
                columns = slice(at * count, (at + 1) * count)
                weights[k * nodes : (k + 1) * nodes, columns] = tall[:nodes]
                ghost_weights[p, k * ghosts : (k + 1) * ghosts, columns] = tall[nodes:]
        acc[p] = jnp.dot(basis_ref[...], weights[...], preferred_element_type=F32)

    def whole_product(p, sums):
        result = acc[p] + jnp.dot(ghost[...], ghost_weights[p], preferred_element_type=F32)
        for at in range(2):
            s = 2 * p + at
            mine = result[:, at * count : (at + 1) * count]
            cols_ref[pl.ds(s, modes, stride=snaps), :] = mine
            norm = jnp.sqrt(jnp.sum(mine * mine, axis=0, keepdims=True))
            norm = jnp.sum(norm, axis=1, keepdims=True)
            line = jnp.concatenate([jnp.sum(mine, axis=1, keepdims=True), norm], axis=0)
            sums = jnp.where(lane == s, line, sums)
        return sums

    pairs = snaps // 2
    if pairs <= 4:
        for p in range(pairs):
            own_product(p)
    else:
        lax.fori_loop(0, pairs, lambda p, c: (own_product(p), c)[1], 0)

    ghost_copy.wait_recv()
    for k in range(3):
        if split:
            ghost[:half, k * ghosts : (k + 1) * ghosts] = ghost_in[k, :, :ghosts]
            ghost[half:, k * ghosts : (k + 1) * ghosts] = ghost_in[k, : modes - half, ghosts:]
        else:
            ghost[:, k * ghosts : (k + 1) * ghosts] = ghost_in[k, :modes]
    sums = jnp.zeros((modes + 1, 128), F32)
    if pairs <= 4:
        for p in range(pairs):
            sums = whole_product(p, sums)
    else:
        sums = lax.fori_loop(0, pairs, whole_product, sums)

    wide = part_p.shape[2]
    part[: modes + 1] = sums
    flat = jnp.concatenate(
        [jnp.transpose(part[t * 128 : (t + 1) * 128])[:snaps] for t in range(wide // 128)], axis=1
    )
    waits = sends + [ghost_copy]

    def reduced(value, ref, me, size, device_of, send, recv):
        ref[me] = value
        arriving = []
        for j, (to, source) in enumerate(peers(me, size)):
            out = remote(ref.at[me], ref.at[me], send.at[j], recv.at[me], device_of(to))
            out.start()
            waits.append(out)
            arriving.append(remote(
                ref.at[source], ref.at[source], send.at[j], recv.at[source], device_of(to)
            ))
        for copy in arriving:
            copy.wait_recv()
        total = ref[0]
        for j in range(1, size):
            total = total + ref[j]
        return total

    flat = reduced(flat, part_p, me_p, params, lambda p: (me_e, p), send_p, recv_p)
    flat = reduced(flat, part_i, me_i, inner, inner_id, send_i, recv_i)
    flat = reduced(flat, part_o, me_o, outer, outer_id, send_o, recv_o)
    flat_ref[...] = flat
    for copy in waits:
        copy.wait_send()


def finish_kernel(elem_total, cols_ref, flat_ref, training_hbm, target_hbm, training, target, sem):
    snaps, modes = target.shape
    row_scale = flat_ref[:, modes : modes + 1] / elem_total
    target[...] = flat_ref[:, :modes] / (row_scale * math.sqrt(elem_total))
    copies = [pltpu.make_async_copy(target, target_hbm, sem.at[0])]
    copies[0].start()
    inverse = jnp.broadcast_to(1.0 / row_scale, (snaps, training.shape[2]))
    chunks = sem.shape[0] - 1
    size = modes // chunks
    for c in range(chunks):
        piece = cols_ref[c * size * snaps : (c + 1) * size * snaps]
        piece = piece.reshape(size, snaps, training.shape[2]) * inverse[None]
        training[c * size : (c + 1) * size] = piece.astype(BF16)
        rows = pl.ds(c * size, size)
        copies.append(pltpu.make_async_copy(training.at[rows], training_hbm.at[rows], sem.at[c + 1]))
        copies[-1].start()
    for copy in copies:
        copy.wait()


def local(elems, params, coords, basis_rows, connectivity, modulus, stiffness):
    own_snaps, modes = coords.shape
    nodes = basis_rows.shape[2]
    count = connectivity.shape[0]
    snaps = own_snaps * params
    ghosts = nodes // 4
    inner = 4 if elems % 4 == 0 else elems
    outer = elems // inner
    half, across = (modes, ghosts) if ghosts % 128 == 0 else (round_up(-(-modes // 2), 32), 2 * ghosts)
    tiles = nodes // 128 + -(-ghosts // 128)
    wide = round_up(modes + 1, 128)
    dma = pltpu.SemaphoreType.DMA
    vmem = pl.BlockSpec(memory_space=pltpu.VMEM)
    hbm = pl.BlockSpec(memory_space=pltpu.HBM)
    dofs = stiffness.shape[0]
    tall = round_up(own_snaps, 8)
    pieces = [
        (stiffness, 0),
        (connectivity.T, dofs),
        (modulus[None], dofs + 8),
        (coords, dofs + 16),
    ]
    height, across_small = dofs + 16 + tall, round_up(max(modes, count), 128)
    small = None
    for piece, at in pieces:
        placed = lax.pad(
            piece, jnp.zeros((), piece.dtype),
            ((at, height - at - piece.shape[0], 0), (0, across_small - piece.shape[1], 0)),
        ).astype(F32)
        small = placed if small is None else small + placed
    cols, flat = pl.pallas_call(
        functools.partial(kernel, elems, params, inner, own_snaps, modes, dofs),
        out_shape=(
            jax.ShapeDtypeStruct((modes * snaps, count), F32),
            jax.ShapeDtypeStruct((snaps, wide), F32),
        ),
        in_specs=[vmem, hbm],
        out_specs=(vmem, vmem),
        scratch_shapes=[
            pltpu.VMEM((modes, 3 * nodes), BF16),
            pltpu.VMEM((3, round_up(half, 16), across), BF16),
            pltpu.VMEM((3, round_up(half, 16), across), BF16),
            pltpu.VMEM((modes, 3 * ghosts), BF16),
            pltpu.VMEM((params, tiles, 3, own_snaps, 128), F32),
            pltpu.VMEM((nodes + ghosts, count), BF16),
            pltpu.VMEM((3 * nodes, 2 * count), BF16),
            pltpu.VMEM((snaps // 2, 3 * ghosts, 2 * count), BF16),
            pltpu.VMEM((snaps // 2, modes, 2 * count), F32),
            pltpu.VMEM((wide, 128), F32),
            pltpu.VMEM((params, snaps, wide), F32),
            pltpu.VMEM((inner, snaps, wide), F32),
            pltpu.VMEM((outer, snaps, wide), F32),
            dma((3,)), dma, dma,
            dma((params,)), dma((params,)),
            dma((params,)), dma((params,)),
            dma((params,)), dma((params,)),
            dma((inner,)), dma((inner,)),
            dma((outer,)), dma((outer,)),
        ],
        compiler_params=pltpu.CompilerParams(
            collective_id=0, has_side_effects=True, vmem_limit_bytes=44 * 1024 * 1024
        ),
    )(small, basis_rows)
    chunks = next(c for c in (4, 3, 2, 1) if modes % c == 0)
    training, target = pl.pallas_call(
        functools.partial(finish_kernel, count * elems * params),
        out_shape=(
            jax.ShapeDtypeStruct((modes, snaps, count), BF16),
            jax.ShapeDtypeStruct((snaps, modes), F32),
        ),
        in_specs=[vmem, vmem],
        out_specs=(hbm, hbm),
        scratch_shapes=[
            pltpu.VMEM((modes, snaps, count), BF16),
            pltpu.VMEM((snaps, modes), F32),
            dma((chunks + 1,)),
        ],
        compiler_params=pltpu.CompilerParams(vmem_limit_bytes=20 * 1024 * 1024),
    )(cols, flat)
    return (jnp.transpose(training, (1, 0, 2)), target)


def solution(mesh):
    in_specs = (
        P("param", None),
        P(None, None, "elem"),
        P(("elem", "param"), None),
        P(("elem", "param")),
        P(),
    )
    out_specs = (P(None, None, ("elem", "param")), P())
    run = functools.partial(local, mesh.shape["elem"], mesh.shape["param"])
    return jax.shard_map(run, mesh=mesh, in_specs=in_specs, out_specs=out_specs, check_vma=False)
```
